16 devices in a mesh: dp: 4 (over y, z, core), ep: 4 (over x).
Axes of the slice: x: 4, y: 2, z: 1, core: 2. Of those that a mesh axis runs over, the one named last changes fastest.
The devices are a block of a 4x4x8 slice.
Arguments:
- x: bfloat16 [4, 4, 256, 2048], P('dp', 'ep'), parts along dimension 0
- expert: int32 [4, 4, 256, 2], P('dp', 'ep'), parts along dimension 0
- slot: int32 [4, 4, 256, 2], P('dp', 'ep'), parts along dimension 0
- gate: float32 [4, 4, 256, 2], P('dp', 'ep'), parts along dimension 0
- w_gate: bfloat16 [8, 2048, 5632], P('ep')
- w_up: bfloat16 [8, 2048, 5632], P('ep')
- w_down: bfloat16 [8, 5632, 2048], P('ep')
Outputs:
- y: bfloat16 [4, 4, 256, 2048], P('dp', 'ep'), parts along dimension 0
There are 4 independent parts. The reference program is written for one: setup_inputs(seed, part) draws one part's arguments, and reference() takes and returns one part's arrays. A program takes and returns all parts, laid end to end along the dimension named above; an argument that names none is the same for every part.
All inputs are finite; a program needn't handle non-finite values.
Results may differ from the reference program's by a relative error of at most 0.009.
Values are sent between devices in bfloat16 or wider.
A program may use at most 768 MiB of HBM per device.

```python
import jax
import jax.numpy as jnp

MEMBERS = 4
TOKENS = 256
D = 2048
FF = 5632
TOP = 2
EXPERTS = 8
SLOTS = 5 * TOKENS * TOP // (4 * EXPERTS)


def setup_inputs(seed: int = 0, part: int = 0) -> dict:
    own, k1, k2, k3, k4, k5, k6 = jax.random.split(jax.random.key(seed), 7)
    kx, ke, kl, kg = jax.random.split(jax.random.fold_in(own, part), 4)
    devices = (1, MEMBERS)
    place = jax.random.permutation(kl, jnp.arange(EXPERTS, dtype=jnp.uint32))
    slow = ((EXPERTS + (9 * place) % EXPERTS) << ((9 * place) // EXPERTS)) // EXPERTS
    wait = (jax.random.bits(ke, (*devices, TOKENS, EXPERTS), jnp.uint32) >> 10) * slow
    expert = jnp.argsort(wait, axis=-1)[..., :TOP].astype(jnp.int32)
    chosen = jax.nn.one_hot(expert, EXPERTS, dtype=jnp.int32)
    in_line = jnp.cumsum(chosen.reshape(*devices, TOKENS * TOP, EXPERTS), axis=2) - 1
    slot = jnp.sum(in_line.reshape(chosen.shape) * chosen, axis=-1)

    def one(key, rows, columns):
        return (jax.random.normal(key, (rows, columns), jnp.float32) * rows**-0.5).astype(jnp.bfloat16)

    def weights(key, rows, columns):
        return jax.lax.map(lambda k: one(k, rows, columns), jax.random.split(key, EXPERTS))

    return {
        "x": jax.random.normal(kx, (*devices, TOKENS, D), jnp.float32).astype(jnp.bfloat16),
        "expert": expert,
        "slot": slot,
        "gate": jax.nn.softmax(jax.random.normal(kg, expert.shape, jnp.float32)),
        "w_gate": weights(k1, D, FF),
        "w_up": weights(k2, D, FF),
        "w_down": weights(k3, FF, D),
    }


def einsum(form, a, b):
    return jnp.einsum(form, a.astype(jnp.float32), b.astype(jnp.float32))


def reference(x, expert, slot, gate, w_gate, w_up, w_down):
    to_expert = jax.nn.one_hot(expert, EXPERTS, dtype=jnp.bfloat16)
    to_slot = jax.nn.one_hot(slot, SLOTS, dtype=jnp.bfloat16)
    weighted = to_expert * gate[..., None].astype(jnp.bfloat16)
    dispatch = einsum("abtke,abtkc->abtec", to_expert, to_slot).astype(jnp.bfloat16)
    combine = einsum("abtke,abtkc->abtec", weighted, to_slot).astype(jnp.bfloat16)
    z = einsum("abtec,abtd->aebcd", dispatch, x).astype(jnp.bfloat16)
    h = jax.nn.silu(einsum("aebcd,edf->aebcf", z, w_gate))
    h = (h * einsum("aebcd,edf->aebcf", z, w_up)).astype(jnp.bfloat16)
    out = einsum("aebcf,efd->aebcd", h, w_down).astype(jnp.bfloat16)
    y = einsum("abtec,aebcd->abtd", combine, out)
    return y.astype(jnp.bfloat16)
```

```python
import functools

import jax
import jax.numpy as jnp
from jax import lax
from jax.experimental import pallas as pl
from jax.experimental.pallas import tpu as pltpu
from jax.sharding import PartitionSpec as P

MESH = pl.DeviceIdType.MESH
PLACE = {0: 0, 2: 1, 1: 2, 3: 3}
DISTANCE = {place: k for k, place in PLACE.items()}
RING = 7
UNIT = 512
TILE = 512
F32 = jnp.float32
BF16 = jnp.bfloat16


def dot(a, b):
    return jnp.dot(a, b, preferred_element_type=F32)


def kernel(slots, info_ref, x_ref, wg, wu, wd, y_ref, zs, zr, h, os, orv, w1, w2, comb,
           w1_sem, w2_sem, zs_sem, zr_sem, os_sem, or_sem, ns_sem, nr_sem, ls_sem, lr_sem):
    tokens, d = x_ref.shape
    ff = h.shape[1]
    pair = 2 * slots
    units, tiles = ff // UNIT, d // TILE
    n = 4
    me, group = lax.axis_index("ep"), lax.axis_index("dp")
    core = lax.rem(group, 2)
    base = group - core

    def device(k, c):
        return {"ep": lax.rem(me + k, n), "dp": base + c}

    def partner():
        return {"ep": me, "dp": base + 1 - core}

    barrier = pltpu.get_barrier_semaphore()
    pl.semaphore_signal(barrier, inc=1, device_id=partner(), device_id_type=MESH)
    for k in range(1, n):
        for c in range(2):
            pl.semaphore_signal(barrier, inc=1, device_id=device(k, c), device_id_type=MESH)

    def w1_copies(unit, slot):
        columns = pl.ds(pl.multiple_of(unit * UNIT, UNIT), UNIT)
        return [
            pltpu.make_async_copy(w.at[core, :, columns], w1.at[slot, i], w1_sem.at[slot, i])
            for i, w in enumerate((wg, wu))
        ]

    def w2_copy(tile, slot):
        columns = pl.ds(pl.multiple_of(tile * TILE, TILE), TILE)
        return pltpu.make_async_copy(wd.at[core, :, columns], w2.at[slot], w2_sem.at[slot])

    def unit_of(turn, p):
        return lax.rem(p + (units - RING) * turn, units)

    def slot_of(turn, p):
        return lax.rem(units * turn + p, RING)

    for p in range(RING):
        for copy in w1_copies(p, p):
            copy.start()

    info = info_ref[...]
    across = jnp.concatenate([info, jnp.zeros((128 - info.shape[0], tokens), F32)], axis=0).T

    def owner(place):
        return (lax.rem(me + DISTANCE[place], n) * pair).astype(F32)

    def dispatch(place):
        row = lax.broadcasted_iota(jnp.int32, (pair, tokens), 0).astype(F32) + owner(place)
        pick = (info[0:1] == row) | (info[1:2] == row)
        pick = jnp.where(pick, 1.0, 0.0).astype(BF16)
        for t in range(d // 512):
            columns = slice(t * 512, (t + 1) * 512)
            zs[place * pair:(place + 1) * pair, columns] = dot(pick, x_ref[:, columns]).astype(BF16)

    def z_copy(place, c):
        k = DISTANCE[place]
        there = PLACE[(n - k) % n]
        return pltpu.make_async_remote_copy(
            src_ref=zs.at[pl.ds(place * pair + c * slots, slots)],
            dst_ref=zr.at[pl.ds(pl.multiple_of(there * pair + core * slots, 16), slots)],
            send_sem=zs_sem.at[place * 2 + c],
            recv_sem=zr_sem.at[there * 2 + core],
            device_id=device(k, c) if k else partner(),
            device_id_type=MESH,
        )

    def arrived(ref, sem):
        pltpu.make_async_remote_copy(
            src_ref=ref, dst_ref=ref, send_sem=sem, recv_sem=sem, device_id=partner(), device_id_type=MESH
        ).wait_recv()

    def z_arrived(place, c):
        arrived(zr.at[pl.ds(place * pair + c * slots, slots)], zr_sem.at[place * 2 + c])

    own = pl.ds(pl.multiple_of(core * slots, 16), slots)
    other = 1 - core
    dispatch(1)
    dispatch(0)
    pl.semaphore_wait(barrier, 2 * n - 1)
    for c in range(2):
        z_copy(1, c).start()
    to_partner = pltpu.make_async_remote_copy(
        src_ref=zs.at[pl.ds(pl.multiple_of(other * slots, 16), slots)],
        dst_ref=zr.at[own],
        send_sem=zs_sem.at[0],
        recv_sem=zr_sem.at[0],
        device_id=partner(),
        device_id_type=MESH,
    )
    to_partner.start()
    zr[own, :] = zs[own, :]
    dispatch(2)
    dispatch(3)
    for place in range(n):
        column = lax.broadcasted_iota(jnp.int32, (tokens, pair), 1).astype(F32) + owner(place)
        weight = jnp.where(across[:, 0:1] == column, across[:, 2:3], 0.0)
        weight = weight + jnp.where(across[:, 1:2] == column, across[:, 3:4], 0.0)
        comb[place] = weight.astype(BF16)
    to_partner.wait_recv()

    def project(turn, p, first, rows):
        slot, unit = slot_of(turn, p), unit_of(turn, p)
        z = zr[first:first + rows, :]
        a = dot(z, w1[slot, 0])
        b = dot(z, w1[slot, 1])
        columns = pl.ds(pl.multiple_of(unit * UNIT, UNIT), UNIT)
        h[first:first + rows, columns] = (a * jax.nn.sigmoid(a) * b).astype(BF16)

    def up_pass(turn, first, rows, extra=None):
        def step(p, _):
            def arrive():
                for copy in w1_copies(unit_of(turn, p), slot_of(turn, p)):
                    copy.wait()

            if turn == 0:
                arrive()
            else:
                pl.when(p >= RING)(arrive)
            project(turn, p, first, rows)

            @pl.when(p < units - RING)
            def _():
                for copy in w1_copies(unit_of(turn, p + RING), slot_of(turn, p)):
                    copy.start()

            if extra is not None:
                extra(p)
            return 0

        lax.fori_loop(0, units, step, 0)

    def first_extra(p):
        @pl.when(p == units - RING)
        def _():
            for tile in range(2):
                w2_copy(tile, tile).start()

        @pl.when(p == SEND_N)
        def _():
            for place in (2, 3):
                for c in range(2):
                    z_copy(place, c).start()

    up_pass(0, 0, pair, first_extra)
    for c in range(2):
        z_arrived(1, c)
    up_pass(1, pair, pair)

    def far_step(i, _):
        slot = lax.rem(i, 2)
        w2_copy(i, slot).wait()
        os[i, pair:2 * pair, :] = dot(h[pair:2 * pair, :], w2[slot]).astype(BF16)

        @pl.when(i < 2)
        def _():
            w2_copy(i + 2, slot).start()

        return 0

    lax.fori_loop(0, tiles, far_step, 0)

    for place in (2, 3):
        for c in range(2):
            z_arrived(place, c)

    def far_copy(c):
        return pltpu.make_async_remote_copy(
            src_ref=os.at[:, pl.ds(pair + c * slots, slots), :],
            dst_ref=orv.at[:, pl.ds(pl.multiple_of(pair + core * slots, 16), slots), :],
            send_sem=os_sem.at[c],
            recv_sem=or_sem.at[core],
            device_id=device(2, c),
            device_id_type=MESH,
        )

    for c in range(2):
        far_copy(c).start()

    up_pass(2, 2 * pair, 2 * pair)

    def near_copy(tile, place, c):
        k = DISTANCE[place]
        there = PLACE[(n - k) % n]
        return pltpu.make_async_remote_copy(
            src_ref=os.at[tile, pl.ds(place * pair + c * slots, slots), :],
            dst_ref=orv.at[tile, pl.ds(pl.multiple_of(there * pair + core * slots, 16), slots), :],
            send_sem=ns_sem.at[tile, (place - 2) * 2 + c],
            recv_sem=nr_sem.at[tile, (there - 2) * 2 + core],
            device_id=device(k, c),
            device_id_type=MESH,
        )

    def partner_copy(tile):
        return pltpu.make_async_remote_copy(
            src_ref=os.at[tile, pl.ds(pl.multiple_of(other * slots, 16), slots), :],
            dst_ref=orv.at[tile, own, :],
            send_sem=ls_sem.at[tile],
            recv_sem=lr_sem.at[tile],
            device_id=partner(),
            device_id_type=MESH,
        )

    def near_step(i, _):
        tile, slot = lax.rem(i + 2, tiles), lax.rem(i, 2)

        @pl.when(i >= 2)
        def _():
            w2_copy(tile, slot).wait()

        os[tile, 2 * pair:4 * pair, :] = dot(h[2 * pair:4 * pair, :], w2[slot]).astype(BF16)
        for place in (2, 3):
            for c in range(2):
                near_copy(tile, place, c).start()
        os[tile, 0:pair, :] = dot(h[0:pair, :], w2[slot]).astype(BF16)
        partner_copy(tile).start()
        orv[tile, own, :] = os[tile, own, :]

        @pl.when(i < 2)
        def _():
            w2_copy(i, slot).start()

        return 0

    lax.fori_loop(0, tiles, near_step, 0)

    for c in range(2):
        arrived(orv.at[:, pl.ds(pair + c * slots, slots), :], or_sem.at[c])
    for i in range(tiles):
        tile = (i + 2) % tiles
        for place in (2, 3):
            for c in range(2):
                rows = pl.ds(place * pair + c * slots, slots)
                arrived(orv.at[tile, rows, :], nr_sem.at[tile, (place - 2) * 2 + c])
        partner_copy(tile).wait_recv()
        total = dot(comb[0], orv[tile, 0:pair, :])
        for place in range(1, n):
            total = total + dot(comb[place], orv[tile, place * pair:(place + 1) * pair, :])
        y_ref[:, tile * TILE:(tile + 1) * TILE] = total.astype(BF16)

    to_partner.wait_send()
    for c in range(2):
        for place in range(1, n):
            z_copy(place, c).wait_send()
        far_copy(c).wait_send()
    for tile in range(tiles):
        partner_copy(tile).wait_send()
        for place in (2, 3):
            for c in range(2):
                near_copy(tile, place, c).wait_send()


SEND_N = 8


def solution(mesh):
    def body(x, expert, slot, gate, w_gate, w_up, w_down):
        tokens, d = x.shape[2:]
        top = expert.shape[3]
        held, _, ff = w_gate.shape
        experts = held * mesh.shape["ep"]
        slots = 5 * tokens * top // (4 * experts)
        rows = experts * slots
        code = jnp.where(slot < slots, expert * slots + slot, -1)[0, 0].T.astype(F32)
        weight = gate.astype(BF16)[0, 0].T.astype(F32)
        info = jnp.concatenate([code, weight, jnp.zeros((4, tokens), F32)], axis=0)
        vmem = pl.BlockSpec(memory_space=pltpu.VMEM)
        hbm = pl.BlockSpec(memory_space=pltpu.HBM)
        tiles = d // TILE
        dma = pltpu.SemaphoreType.DMA
        y = pl.pallas_call(
            functools.partial(kernel, slots),
            name="moe",
            out_shape=jax.ShapeDtypeStruct((tokens, d), BF16),
            in_specs=[vmem, vmem, hbm, hbm, hbm],
            out_specs=vmem,
            scratch_shapes=[
                pltpu.VMEM((rows, d), BF16),
                pltpu.VMEM((rows, d), BF16),
                pltpu.VMEM((rows, ff), BF16),
                pltpu.VMEM((tiles, rows, TILE), BF16),
                pltpu.VMEM((tiles, rows, TILE), BF16),
                pltpu.VMEM((RING, 2, d, UNIT), BF16),
                pltpu.VMEM((2, ff, TILE), BF16),
                pltpu.VMEM((4, tokens, 2 * slots), BF16),
                dma((RING, 2)),
                dma((2,)),
                dma((8,)),
                dma((8,)),
                dma((2,)),
                dma((2,)),
                dma((tiles, 4)),
                dma((tiles, 4)),
                dma((tiles,)),
                dma((tiles,)),
            ],
            compiler_params=pltpu.CompilerParams(
                collective_id=0, has_side_effects=True, vmem_limit_bytes=67_000_000
            ),
        )(info, x[0, 0], w_gate, w_up, w_down)
        return y[None, None]

    part = P("dp", "ep")
    weights = P("ep")
    return jax.shard_map(
        body, mesh=mesh, in_specs=(part, part, part, part, weights, weights, weights), out_specs=part, check_vma=False
    )
```

```python
import functools

import jax
import jax.numpy as jnp
from jax import lax
from jax.experimental import pallas as pl
from jax.experimental.pallas import tpu as pltpu
from jax.sharding import PartitionSpec as P

MESH = pl.DeviceIdType.MESH
MEMBERS = 4
BLOCKS = [(0, 0), (0, 1), (1, 0), (3, 0), (2, 0), (2, 1), (1, 1), (3, 1)]
L, N1, O, N2 = range(4)
RING = 7
UNIT = 512
TILE = 512
F32 = jnp.float32
BF16 = jnp.bfloat16


def there(block):
    k, rel = BLOCKS[block]
    return BLOCKS.index(((MEMBERS - k) % MEMBERS, rel))


def dot(a, b):
    return jnp.dot(a, b, preferred_element_type=F32)


def kernel(slots, expert, slot, gate, x_hbm, wg, wu, wd, y_ref, x, zs, zr, h, os, orv, w1, w2, comb,
           x_sem, w1_sem, w2_sem, zs_sem, zr_sem, os_sem, or_sem):
    tokens, d = x.shape
    ff = h.shape[1]
    pair = 2 * slots
    units, tiles = ff // UNIT, d // TILE
    me, group = lax.axis_index("ep"), lax.axis_index("dp")
    core = lax.rem(group, 2)
    base = group - core
    cores = (core, 1 - core)

    def device(block):
        k, rel = BLOCKS[block]
        return {"ep": lax.rem(me + k, MEMBERS), "dp": base + cores[rel]}

    def first_code(block):
        k, rel = BLOCKS[block]
        return (2 * lax.rem(me + k, MEMBERS) + cores[rel]) * slots

    def rows(block):
        return pl.ds(block * slots, slots)

    def chunk(c):
        return slice(c * pair, (c + 1) * pair)

    def columns(t, width):
        return pl.ds(pl.multiple_of(t * width, width), width)

    def x_copy(t):
        return pltpu.make_async_copy(x_hbm.at[:, columns(t, TILE)], x.at[:, columns(t, TILE)], x_sem.at[t])

    def w1_start(unit, at):
        for i, w in enumerate((wg, wu)):
            pltpu.make_async_copy(w.at[core, :, columns(unit, UNIT)], w1.at[at, i], w1_sem.at[at, i]).start()

    def w1_wait(at):
        for i in range(2):
            pltpu.make_async_copy(w1.at[at, i], w1.at[at, i], w1_sem.at[at, i]).wait()

    def w2_copy(tile, at):
        return pltpu.make_async_copy(wd.at[core, :, columns(tile, TILE)], w2.at[at], w2_sem.at[at])

    def z_copy(block):
        return pltpu.make_async_remote_copy(
            src_ref=zs.at[rows(block)],
            dst_ref=zr.at[rows(there(block))],
            send_sem=zs_sem.at[block],
            recv_sem=zr_sem.at[there(block)],
            device_id=device(block),
            device_id_type=MESH,
        )

    def o_copy(tile, block):
        return pltpu.make_async_remote_copy(
            src_ref=os.at[tile, rows(block)],
            dst_ref=orv.at[tile, rows(there(block))],
            send_sem=os_sem.at[tile, block],
            recv_sem=or_sem.at[tile, there(block)],
            device_id=device(block),
            device_id_type=MESH,
        )

    def z_arrived(block):
        ref, sem = zr.at[rows(block)], zr_sem.at[block]
        pltpu.make_async_copy(ref, ref, sem).wait()

    def o_arrived(tile, block):
        ref, sem = orv.at[tile, rows(block)], or_sem.at[tile, block]
        pltpu.make_async_copy(ref, ref, sem).wait()

    for t in range(tiles):
        x_copy(t).start()
    barrier = pltpu.get_barrier_semaphore()
    for block in range(1, len(BLOCKS)):
        pl.semaphore_signal(barrier, inc=1, device_id=device(block), device_id_type=MESH)
    for p in range(RING):
        w1_start(p, p)

    code = jnp.where(slot[...] < slots, expert[...] * slots + slot[...], -1)

    def bases(index, c):
        return index + jnp.where(index < slots, first_code(2 * c), first_code(2 * c + 1) - slots)

    def dispatch(c):
        row = bases(lax.broadcasted_iota(jnp.int32, (pair, tokens), 0), c)
        pick = (code[0:1] == row) | (code[1:2] == row)
        pick = jnp.where(pick, 1.0, 0.0).astype(BF16)
        for t in range(tiles):
            if c == N1:
                x_copy(t).wait()
            at = slice(t * TILE, (t + 1) * TILE)
            z = dot(pick, x[:, at]).astype(BF16)
            if c == L:
                zr[0:slots, at] = z[0:slots]
                zs[slots:pair, at] = z[slots:pair]
            else:
                zs[chunk(c), at] = z

    dispatch(N1)
    dispatch(L)
    pl.semaphore_wait(barrier, len(BLOCKS) - 1)
    z_copy(2 * N1).start()
    z_copy(2 * N1 + 1).start()
    z_copy(2 * L + 1).start()
    dispatch(O)
    z_copy(2 * O).start()
    z_copy(2 * O + 1).start()
    dispatch(N2)

    table = jnp.concatenate([code.astype(F32), gate[...], jnp.zeros((124, tokens), F32)], axis=0).T
    for c in range(4):
        column = bases(lax.broadcasted_iota(jnp.int32, (tokens, pair), 1), c).astype(F32)
        weight = jnp.where(table[:, 0:1] == column, table[:, 2:3], 0.0)
        weight = weight + jnp.where(table[:, 1:2] == column, table[:, 3:4], 0.0)
        comb[c] = weight.astype(BF16)

    fresh = units - RING

    def up_pass(turn, c, extra=None):
        def place(p):
            return lax.rem(units * turn + p, RING)

        def unit_of(p):
            return lax.rem(p + fresh * turn, units)

        def project(p):
            at = place(p)
            z = zr[chunk(c), :]
            a = dot(z, w1[at, 0])
            b = dot(z, w1[at, 1])
            h[chunk(c), columns(unit_of(p), UNIT)] = (a * jax.nn.sigmoid(a) * b).astype(BF16)

        def step(i, _):
            for p in (2 * i, 2 * i + 1):
                if turn == 0:
                    w1_wait(place(p))
                else:
                    pl.when(p >= RING)(functools.partial(w1_wait, place(p)))
            for p in (2 * i, 2 * i + 1):
                project(p)

            @pl.when(i < fresh // 2)
            def _():
                for p in (2 * i, 2 * i + 1):
                    w1_start(unit_of(p + RING), place(p))

            if extra is not None:
                extra(i)
            return 0

        lax.fori_loop(0, units // 2, step, 0)
        w1_wait(place(units - 1))
        project(units - 1)

    def down_pass(turn, c):
        def step(i, _):
            tile, at = lax.rem(i + 2 * turn, tiles), lax.rem(i, 2)
            if turn == 0:
                w2_copy(tile, at).wait()
            else:
                pl.when(i >= 2)(lambda: w2_copy(tile, at).wait())
            out = dot(h[chunk(c), :], w2[at]).astype(BF16)
            if c == L:
                orv[tile, 0:slots, :] = out[0:slots]
                os[tile, slots:pair, :] = out[slots:pair]
            else:
                os[tile, chunk(c), :] = out
                o_copy(tile, 2 * c).start()
            o_copy(tile, 2 * c + 1).start()

            @pl.when(i < 2)
            def _():
                w2_copy(lax.rem(i + 2 + 2 * turn, tiles), at).start()

            return 0

        lax.fori_loop(0, tiles, step, 0)

    def load_down(i):
        @pl.when(i == fresh // 2)
        def _():
            for tile in range(2):
                w2_copy(tile, tile).start()

    def send_n2(i):
        @pl.when(i == SEND_N2)
        def _():
            z_copy(2 * N2).start()
            z_copy(2 * N2 + 1).start()

    def wait_z(c):
        z_arrived(2 * c)
        z_arrived(2 * c + 1)

    z_arrived(2 * L + 1)
    up_pass(0, L, load_down)
    wait_z(N1)
    up_pass(1, N1, send_n2)
    down_pass(0, N1)
    wait_z(O)
    up_pass(2, O)
    down_pass(1, O)
    wait_z(N2)
    up_pass(3, N2)
    down_pass(2, N2)
    down_pass(3, L)

    for tile in range(tiles):
        for block in range(1, len(BLOCKS)):
            o_arrived(tile, block)
        total = dot(comb[0], orv[tile, chunk(0), :])
        for c in range(1, 4):
            total = total + dot(comb[c], orv[tile, chunk(c), :])
        y_ref[:, tile * TILE:(tile + 1) * TILE] = total.astype(BF16)

    for block in range(1, len(BLOCKS)):
        z_copy(block).wait_send()
        for tile in range(tiles):
            o_copy(tile, block).wait_send()


SEND_N2 = 3


def solution(mesh):
    def body(x, expert, slot, gate, w_gate, w_up, w_down):
        tokens, d = x.shape[2:]
        top = expert.shape[3]
        held, _, ff = w_gate.shape
        experts = held * mesh.shape["ep"]
        slots = 5 * tokens * top // (4 * experts)
        rows = experts * slots
        vmem = pl.BlockSpec(memory_space=pltpu.VMEM)
        hbm = pl.BlockSpec(memory_space=pltpu.HBM)
        tiles = d // TILE
        dma = pltpu.SemaphoreType.DMA
        y = pl.pallas_call(
            functools.partial(kernel, slots),
            name="moe",
            out_shape=OUT((tokens, d), BF16),
            in_specs=[vmem, vmem, vmem, hbm, hbm, hbm, hbm],
            out_specs=vmem,
            scratch_shapes=[
                pltpu.VMEM((tokens, d), BF16),
                pltpu.VMEM((rows, d), BF16),
                pltpu.VMEM((rows, d), BF16),
                pltpu.VMEM((rows, ff), BF16),
                pltpu.VMEM((tiles, rows, TILE), BF16),
                pltpu.VMEM((tiles, rows, TILE), BF16),
                pltpu.VMEM((RING, 2, d, UNIT), BF16),
                pltpu.VMEM((2, ff, TILE), BF16),
                pltpu.VMEM((4, tokens, 2 * slots), BF16),
                dma((tiles,)),
                dma((RING, 2)),
                dma((2,)),
                dma((8,)),
                dma((8,)),
                dma((tiles, 8)),
                dma((tiles, 8)),
            ],
            compiler_params=pltpu.CompilerParams(
                collective_id=0, has_side_effects=True, vmem_limit_bytes=LIMIT
            ),
        )(expert[0, 0].T, slot[0, 0].T, gate[0, 0].T, x[0, 0], w_gate, w_up, w_down)
        return y[None, None]

    part = P("dp", "ep")
    weights = P("ep")
    return jax.shard_map(
        body, mesh=mesh, in_specs=(part, part, part, part, weights, weights, weights), out_specs=part, check_vma=False
    )


OUT = pltpu.VMEM
LIMIT = 65_800_000
```

```python
import functools

import jax
import jax.numpy as jnp
from jax import lax
from jax.experimental import pallas as pl
from jax.experimental.pallas import tpu as pltpu
from jax.sharding import PartitionSpec as P

MESH = pl.DeviceIdType.MESH
MEMBERS = 4
BLOCKS = [(0, 0), (0, 1), (1, 0), (3, 0), (2, 0), (2, 1), (1, 1), (3, 1)]
L, N1, O, N2 = range(4)
RING = 7
UNIT = 512
TILE = 512
F32 = jnp.float32
BF16 = jnp.bfloat16


def there(block):
    k, rel = BLOCKS[block]
    return BLOCKS.index(((MEMBERS - k) % MEMBERS, rel))


def dot(a, b):
    return jnp.dot(a, b, preferred_element_type=F32)


def kernel(slots, expert, slot, gate, x_hbm, wg, wu, wd, y_ref, zs, zr, h, orv, w1, w2,
           x_sem, w1_sem, w2_sem, zs_sem, zr_sem, os_sem, or_sem):
    tokens, d = y_ref.shape
    ff = h.shape[1]
    pair = 2 * slots
    units, tiles = ff // UNIT, d // TILE
    me, group = lax.axis_index("ep"), lax.axis_index("dp")
    core = lax.rem(group, 2)
    base = group - core
    cores = (core, 1 - core)

    def device(block):
        k, rel = BLOCKS[block]
        return {"ep": lax.rem(me + k, MEMBERS), "dp": base + cores[rel]}

    def first_code(block):
        k, rel = BLOCKS[block]
        return (2 * lax.rem(me + k, MEMBERS) + cores[rel]) * slots

    def rows(block):
        return pl.ds(block * slots, slots)

    def chunk(c):
        return slice(c * pair, (c + 1) * pair)

    def columns(t, width):
        return pl.ds(pl.multiple_of(t * width, width), width)

    def sent(c):
        return slice(c * pair - slots, (c + 1) * pair - slots)

    def hidden(c):
        return slice(0, pair) if c == L else slice(pair, 2 * pair)

    def x_copy(t):
        return pltpu.make_async_copy(x_hbm.at[:, columns(t, TILE)], y_ref.at[:, columns(t, TILE)], x_sem.at[t])

    def w1_start(unit, at):
        for i, w in enumerate((wg, wu)):
            pltpu.make_async_copy(w.at[core, :, columns(unit, UNIT)], w1.at[at, i], w1_sem.at[at, i]).start()

    def w1_wait(at):
        for i in range(2):
            pltpu.make_async_copy(w1.at[at, i], w1.at[at, i], w1_sem.at[at, i]).wait()

    def w2_copy(tile):
        return pltpu.make_async_copy(wd.at[core, :, columns(tile, TILE)], w2.at[tile], w2_sem.at[tile])

    def z_copy(block):
        return pltpu.make_async_remote_copy(
            src_ref=zs.at[rows(block - 1)],
            dst_ref=zr.at[rows(there(block))],
            send_sem=zs_sem.at[block],
            recv_sem=zr_sem.at[there(block)],
            device_id=device(block),
            device_id_type=MESH,
        )

    def o_copy(tile, block):
        return pltpu.make_async_remote_copy(
            src_ref=zs.at[rows(block - 1), columns(tile, TILE)],
            dst_ref=orv.at[tile, rows(there(block))],
            send_sem=os_sem.at[tile, block],
            recv_sem=or_sem.at[tile, there(block)],
            device_id=device(block),
            device_id_type=MESH,
        )

    def z_arrived(block):
        ref, sem = zr.at[rows(block)], zr_sem.at[block]
        pltpu.make_async_copy(ref, ref, sem).wait()

    def o_arrived(tile, block):
        ref, sem = orv.at[tile, rows(block)], or_sem.at[tile, block]
        pltpu.make_async_copy(ref, ref, sem).wait()

    for t in range(tiles):
        x_copy(t).start()
    barrier = pltpu.get_barrier_semaphore()
    for block in range(1, len(BLOCKS)):
        pl.semaphore_signal(barrier, inc=1, device_id=device(block), device_id_type=MESH)
    for p in range(RING):
        w1_start(p, p)

    code = jnp.where(slot[...] < slots, expert[...] * slots + slot[...], -1)

    def bases(index, c):
        return index + jnp.where(index < slots, first_code(2 * c), first_code(2 * c + 1) - slots)

    def dispatch(c):
        row = bases(lax.broadcasted_iota(jnp.int32, (pair, tokens), 0), c)
        pick = (code[0:1] == row) | (code[1:2] == row)
        pick = jnp.where(pick, 1.0, 0.0).astype(BF16)
        for t in range(tiles):
            if c == N1:
                x_copy(t).wait()
            at = slice(t * TILE, (t + 1) * TILE)
            z = dot(pick, y_ref[:, at]).astype(BF16)
            if c == L:
                zr[0:slots, at] = z[0:slots]
                zs[0:slots, at] = z[slots:pair]
            else:
                zs[sent(c), at] = z

    dispatch(N1)
    dispatch(L)
    pl.semaphore_wait(barrier, len(BLOCKS) - 1)
    z_copy(2 * N1).start()
    z_copy(2 * N1 + 1).start()
    z_copy(2 * L + 1).start()
    dispatch(O)
    z_copy(2 * O).start()
    z_copy(2 * O + 1).start()
    fresh = units - RING

    def project(at, unit, first, count, into):
        z = zr[first:first + count, :]
        a = dot(z, w1[at, 0])
        b = dot(z, w1[at, 1])
        h[into:into + count, columns(unit, UNIT)] = (a * jax.nn.sigmoid(a) * b).astype(BF16)

    def up_pass(turn, c):
        def place(p):
            return lax.rem(units * turn + p, RING)

        def unit_of(p):
            return lax.rem(p + fresh * turn, units)

        def step(i, _):
            for p in (2 * i, 2 * i + 1):
                pl.when(p >= RING)(functools.partial(w1_wait, place(p)))
            for p in (2 * i, 2 * i + 1):
                project(place(p), unit_of(p), c * pair, pair, pair)

            @pl.when(i < fresh // 2)
            def _():
                for p in (2 * i, 2 * i + 1):
                    w1_start(unit_of(p + RING), place(p))

            return 0

        lax.fori_loop(0, units // 2, step, 0)
        w1_wait(place(units - 1))
        project(place(units - 1), unit_of(units - 1), c * pair, pair, pair)

    def first_own(p, _):
        w1_wait(p)
        project(p, p, 0, pair, 0)
        return 0

    def first_near(i, _):
        for p in (2 * i, 2 * i + 1):
            project(p, p, pair, pair, pair)

        @pl.when(i < fresh // 2)
        def _():
            for p in (2 * i, 2 * i + 1):
                w1_start(p + RING, p)

        return 0

    def first_both(p, _):
        w1_wait(p)
        for c in (L, N1):
            project(p, p + RING, c * pair, pair, c * pair)

        @pl.when(p == SEND_N2)
        def _():
            z_copy(2 * N2).start()
            z_copy(2 * N2 + 1).start()

        return 0

    def down_pass(c, first=False):
        for block in (2 * c, 2 * c + 1):
            if block:
                z_copy(block).wait_send()

        for start in range(0, tiles, BATCH):
            batch = range(start, start + BATCH)
            for tile in batch:
                if first:
                    w2_copy(tile).wait()
            for tile in batch:
                out = dot(h[hidden(c), :], w2[tile]).astype(BF16)
                if c == L:
                    orv[tile, 0:slots, :] = out[0:slots]
                    zs[0:slots, columns(tile, TILE)] = out[slots:pair]
                else:
                    zs[sent(c), columns(tile, TILE)] = out
            for tile in batch:
                if c != L:
                    o_copy(tile, 2 * c).start()
                o_copy(tile, 2 * c + 1).start()

    def wait_z(c):
        z_arrived(2 * c)
        z_arrived(2 * c + 1)

    for tile in range(tiles):
        w2_copy(tile).start(priority=1)
    z_arrived(2 * L + 1)
    lax.fori_loop(0, RING, first_own, 0)
    dispatch(N2)

    wait_z(N1)
    lax.fori_loop(0, RING // 2, first_near, 0)
    project(RING - 1, RING - 1, pair, pair, pair)
    lax.fori_loop(0, fresh, first_both, 0)
    down_pass(N1, first=True)
    def weighs(c, part):
        half = tokens // 2
        at = (2 * c + part) * half * 2
        return slice(pair, pair + half), slice(at, at + pair)

    table = jnp.concatenate([code.astype(F32), gate[...], jnp.zeros((124, tokens), F32)], axis=0).T
    for c in range(4):
        column = bases(lax.broadcasted_iota(jnp.int32, (tokens, pair), 1), c).astype(F32)
        weight = jnp.where(table[:, 0:1] == column, table[:, 2:3], 0.0)
        weight = weight + jnp.where(table[:, 1:2] == column, table[:, 3:4], 0.0)
        weight = weight.astype(BF16)
        for part in range(2):
            zr[weighs(c, part)] = weight[part * (tokens // 2):(part + 1) * (tokens // 2)]

    wait_z(O)
    up_pass(1, O)
    down_pass(O)
    wait_z(N2)
    up_pass(2, N2)
    down_pass(N2)
    down_pass(L)

    for tile in range(tiles):
        for block in range(1, len(BLOCKS)):
            o_arrived(tile, block)
        for part in range(2):
            total = dot(zr[weighs(0, part)], orv[tile, chunk(0), :])
            for c in range(1, 4):
                total = total + dot(zr[weighs(c, part)], orv[tile, chunk(c), :])
            half = tokens // 2
            y_ref[part * half:(part + 1) * half, tile * TILE:(tile + 1) * TILE] = total.astype(BF16)

    for block in range(1, len(BLOCKS)):
        for tile in range(tiles):
            o_copy(tile, block).wait_send()


SEND_N2 = 1
BATCH = 2


def solution(mesh):
    def body(x, expert, slot, gate, w_gate, w_up, w_down):
        tokens, d = x.shape[2:]
        top = expert.shape[3]
        held, _, ff = w_gate.shape
        experts = held * mesh.shape["ep"]
        slots = 5 * tokens * top // (4 * experts)
        rows = experts * slots
        vmem = pl.BlockSpec(memory_space=pltpu.VMEM)
        hbm = pl.BlockSpec(memory_space=pltpu.HBM)
        tiles = d // TILE
        dma = pltpu.SemaphoreType.DMA
        y = pl.pallas_call(
            functools.partial(kernel, slots),
            name="moe",
            out_shape=OUT((tokens, d), BF16),
            in_specs=[vmem, vmem, vmem, hbm, hbm, hbm, hbm],
            out_specs=vmem,
            scratch_shapes=[
                pltpu.VMEM((rows - slots, d), BF16),
                pltpu.VMEM((rows, d), BF16),
                pltpu.VMEM((4 * slots, ff), BF16),
                pltpu.VMEM((tiles, rows, TILE), BF16),
                pltpu.VMEM((RING, 2, d, UNIT), BF16),
                pltpu.VMEM((tiles, ff, TILE), BF16),
                dma((tiles,)),
                dma((RING, 2)),
                dma((tiles,)),
                dma((8,)),
                dma((8,)),
                dma((tiles, 8)),
                dma((tiles, 8)),
            ],
            compiler_params=pltpu.CompilerParams(
                collective_id=0, has_side_effects=True, vmem_limit_bytes=LIMIT
            ),
        )(expert[0, 0].T, slot[0, 0].T, gate[0, 0].T, x[0, 0], w_gate, w_up, w_down)
        return y[None, None]

    part = P("dp", "ep")
    weights = P("ep")
    return jax.shard_map(
        body, mesh=mesh, in_specs=(part, part, part, part, weights, weights, weights), out_specs=part, check_vma=False
    )


OUT = pltpu.VMEM
LIMIT = 65_800_000
```

```python
import functools

import jax
import jax.numpy as jnp
from jax import lax
from jax.experimental import pallas as pl
from jax.experimental.pallas import tpu as pltpu
from jax.sharding import PartitionSpec as P

MESH = pl.DeviceIdType.MESH
MEMBERS = 4
BLOCKS = [(0, 0), (0, 1), (1, 0), (3, 0), (2, 0), (2, 1), (1, 1), (3, 1)]
L, N1, O, N2 = range(4)
RING = 7
UNIT = 512
TILE = 512
F32 = jnp.float32
BF16 = jnp.bfloat16


def there(block):
    k, rel = BLOCKS[block]
    return BLOCKS.index(((MEMBERS - k) % MEMBERS, rel))


def dot(a, b):
    return jnp.dot(a, b, preferred_element_type=F32)


def kernel(slots, expert, slot, gate, x_hbm, wg, wu, wd, y_ref, zs, zr, h, orv, w1, w2,
           x_sem, w1_sem, w2_sem, zs_sem, zr_sem, os_sem, or_sem):
    tokens, d = y_ref.shape
    ff = h.shape[1]
    pair = 2 * slots
    units, tiles = ff // UNIT, d // TILE
    me, group = lax.axis_index("ep"), lax.axis_index("dp")
    core = lax.rem(group, 2)
    base = group - core
    cores = (core, 1 - core)

    def device(block):
        k, rel = BLOCKS[block]
        return {"ep": lax.rem(me + k, MEMBERS), "dp": base + cores[rel]}

    def first_code(block):
        k, rel = BLOCKS[block]
        return (2 * lax.rem(me + k, MEMBERS) + cores[rel]) * slots

    def rows(block):
        return pl.ds(block * slots, slots)

    def chunk(c):
        return slice(c * pair, (c + 1) * pair)

    def columns(t, width):
        return pl.ds(pl.multiple_of(t * width, width), width)

    def sent(c):
        return slice(c * pair - slots, (c + 1) * pair - slots)

    def hidden(c):
        return slice(0, pair) if c == L else slice(pair, 2 * pair)

    def x_copy(t):
        return pltpu.make_async_copy(x_hbm.at[:, columns(t, TILE)], y_ref.at[:, columns(t, TILE)], x_sem.at[t])

    def w1_start(unit, at):
        for i, w in enumerate((wg, wu)):
            pltpu.make_async_copy(w.at[core, :, columns(unit, UNIT)], w1.at[at, i], w1_sem.at[at, i]).start()

    def w1_wait(at):
        for i in range(2):
            pltpu.make_async_copy(w1.at[at, i], w1.at[at, i], w1_sem.at[at, i]).wait()

    def w2_copy(tile):
        return pltpu.make_async_copy(wd.at[core, :, columns(tile, TILE)], w2.at[tile], w2_sem.at[tile])

    def z_copy(block):
        return pltpu.make_async_remote_copy(
            src_ref=zs.at[rows(block - 1)],
            dst_ref=zr.at[rows(there(block))],
            send_sem=zs_sem.at[block],
            recv_sem=zr_sem.at[there(block)],
            device_id=device(block),
            device_id_type=MESH,
        )

    def o_copy(tile, block):
        return pltpu.make_async_remote_copy(
            src_ref=zs.at[rows(block - 1), columns(tile, TILE)],
            dst_ref=orv.at[tile, rows(there(block))],
            send_sem=os_sem.at[tile, block],
            recv_sem=or_sem.at[tile, there(block)],
            device_id=device(block),
            device_id_type=MESH,
        )

    def z_arrived(block):
        ref, sem = zr.at[rows(block)], zr_sem.at[block]
        pltpu.make_async_copy(ref, ref, sem).wait()

    def o_arrived(tile, block):
        ref, sem = orv.at[tile, rows(block)], or_sem.at[tile, block]
        pltpu.make_async_copy(ref, ref, sem).wait()

    for t in range(tiles):
        x_copy(t).start()
    barrier = pltpu.get_barrier_semaphore()
    for block in range(1, len(BLOCKS)):
        pl.semaphore_signal(barrier, inc=1, device_id=device(block), device_id_type=MESH)
    for p in range(RING):
        w1_start(p, p)

    code = jnp.where(slot[...] < slots, expert[...] * slots + slot[...], -1)

    def bases(index, c):
        return index + jnp.where(index < slots, first_code(2 * c), first_code(2 * c + 1) - slots)

    def dispatch(c):
        row = bases(lax.broadcasted_iota(jnp.int32, (pair, tokens), 0), c)
        pick = (code[0:1] == row) | (code[1:2] == row)
        pick = jnp.where(pick, 1.0, 0.0).astype(BF16)
        for t in range(tiles):
            if c == N1:
                x_copy(t).wait()
            at = slice(t * TILE, (t + 1) * TILE)
            z = dot(pick, y_ref[:, at]).astype(BF16)
            if c == L:
                zr[0:slots, at] = z[0:slots]
                zs[0:slots, at] = z[slots:pair]
            else:
                zs[sent(c), at] = z

    dispatch(N1)
    pl.semaphore_wait(barrier, len(BLOCKS) - 1)
    z_copy(2 * N1).start()
    z_copy(2 * N1 + 1).start()
    dispatch(L)
    dispatch(O)
    z_copy(2 * L + 1).start()
    z_copy(2 * O).start()
    z_copy(2 * O + 1).start()
    fresh = units - RING

    def project(at, unit, first, count, into):
        z = zr[first:first + count, :]
        a = dot(z, w1[at, 0])
        b = dot(z, w1[at, 1])
        h[into:into + count, columns(unit, UNIT)] = (a * jax.nn.sigmoid(a) * b).astype(BF16)

    def up_pass(turn, c):
        def place(p):
            return lax.rem(units * turn + p, RING)

        def unit_of(p):
            return lax.rem(p + fresh * turn, units)

        def step(i, _):
            for p in (2 * i, 2 * i + 1):
                pl.when(p >= RING)(functools.partial(w1_wait, place(p)))
            for p in (2 * i, 2 * i + 1):
                project(place(p), unit_of(p), c * pair, pair, pair)

            @pl.when(i < fresh // 2)
            def _():
                for p in (2 * i, 2 * i + 1):
                    w1_start(unit_of(p + RING), place(p))

            return 0

        lax.fori_loop(0, units // 2, step, 0)
        w1_wait(place(units - 1))
        project(place(units - 1), unit_of(units - 1), c * pair, pair, pair)

    def first_own(p, _):
        w1_wait(p)
        project(p, p, 0, pair, 0)
        return 0

    def first_near(i, _):
        for p in (2 * i, 2 * i + 1):
            project(p, p, pair, pair, pair)

        @pl.when(i < fresh // 2)
        def _():
            for p in (2 * i, 2 * i + 1):
                w1_start(p + RING, p)

        return 0

    def first_both(p, _):
        w1_wait(p)
        for c in (L, N1):
            project(p, p + RING, c * pair, pair, c * pair)

        @pl.when(p == SEND_N2)
        def _():
            z_copy(2 * N2).start()
            z_copy(2 * N2 + 1).start()

        return 0

    def down_pass(c, first=False):
        for block in (2 * c, 2 * c + 1):
            if block:
                z_copy(block).wait_send()

        for start in range(0, tiles, BATCH):
            batch = range(start, start + BATCH)
            for tile in batch:
                if first:
                    w2_copy(tile).wait()
            for tile in batch:
                out = dot(h[hidden(c), :], w2[tile]).astype(BF16)
                if c == L:
                    orv[tile, 0:slots, :] = out[0:slots]
                    zs[0:slots, columns(tile, TILE)] = out[slots:pair]
                else:
                    zs[sent(c), columns(tile, TILE)] = out
            for tile in batch:
                if c != L:
                    o_copy(tile, 2 * c).start()
                o_copy(tile, 2 * c + 1).start()

    def wait_z(c):
        z_arrived(2 * c)
        z_arrived(2 * c + 1)

    for tile in range(tiles):
        w2_copy(tile).start(priority=1)
    z_arrived(2 * L + 1)
    lax.fori_loop(0, RING, first_own, 0)
    dispatch(N2)

    wait_z(N1)
    lax.fori_loop(0, RING // 2, first_near, 0)
    project(RING - 1, RING - 1, pair, pair, pair)
    lax.fori_loop(0, fresh, first_both, 0)
    down_pass(N1, first=True)
    def weighs(c, part):
        half = tokens // 2
        at = (2 * c + part) * half * 2
        return slice(pair, pair + half), slice(at, at + pair)

    table = jnp.concatenate([code.astype(F32), gate[...], jnp.zeros((124, tokens), F32)], axis=0).T
    for c in range(4):
        column = bases(lax.broadcasted_iota(jnp.int32, (tokens, pair), 1), c).astype(F32)
        weight = jnp.where(table[:, 0:1] == column, table[:, 2:3], 0.0)
        weight = weight + jnp.where(table[:, 1:2] == column, table[:, 3:4], 0.0)
        weight = weight.astype(BF16)
        for part in range(2):
            zr[weighs(c, part)] = weight[part * (tokens // 2):(part + 1) * (tokens // 2)]

    wait_z(O)
    up_pass(1, O)
    down_pass(O)
    wait_z(N2)
    up_pass(2, N2)
    down_pass(N2)
    down_pass(L)

    for tile in range(tiles):
        for block in range(1, len(BLOCKS)):
            o_arrived(tile, block)
        for part in range(2):
            total = dot(zr[weighs(0, part)], orv[tile, chunk(0), :])
            for c in range(1, 4):
                total = total + dot(zr[weighs(c, part)], orv[tile, chunk(c), :])
            half = tokens // 2
            y_ref[part * half:(part + 1) * half, tile * TILE:(tile + 1) * TILE] = total.astype(BF16)

    for block in range(1, len(BLOCKS)):
        for tile in range(tiles):
            o_copy(tile, block).wait_send()


SEND_N2 = 1
BATCH = 1


def solution(mesh):
    def body(x, expert, slot, gate, w_gate, w_up, w_down):
        tokens, d = x.shape[2:]
        top = expert.shape[3]
        held, _, ff = w_gate.shape
        experts = held * mesh.shape["ep"]
        slots = 5 * tokens * top // (4 * experts)
        rows = experts * slots
        vmem = pl.BlockSpec(memory_space=pltpu.VMEM)
        hbm = pl.BlockSpec(memory_space=pltpu.HBM)
        tiles = d // TILE
        dma = pltpu.SemaphoreType.DMA
        y = pl.pallas_call(
            functools.partial(kernel, slots),
            name="moe",
            out_shape=OUT((tokens, d), BF16),
            in_specs=[vmem, vmem, vmem, hbm, hbm, hbm, hbm],
            out_specs=vmem,
            scratch_shapes=[
                pltpu.VMEM((rows - slots, d), BF16),
                pltpu.VMEM((rows, d), BF16),
                pltpu.VMEM((4 * slots, ff), BF16),
                pltpu.VMEM((tiles, rows, TILE), BF16),
                pltpu.VMEM((RING, 2, d, UNIT), BF16),
                pltpu.VMEM((tiles, ff, TILE), BF16),
                dma((tiles,)),
                dma((RING, 2)),
                dma((tiles,)),
                dma((8,)),
                dma((8,)),
                dma((tiles, 8)),
                dma((tiles, 8)),
            ],
            compiler_params=pltpu.CompilerParams(
                collective_id=0, has_side_effects=True, vmem_limit_bytes=LIMIT
            ),
        )(expert[0, 0].T, slot[0, 0].T, gate[0, 0].T, x[0, 0], w_gate, w_up, w_down)
        return y[None, None]

    part = P("dp", "ep")
    weights = P("ep")
    return jax.shard_map(
        body, mesh=mesh, in_specs=(part, part, part, part, weights, weights, weights), out_specs=part, check_vma=False
    )


OUT = pltpu.VMEM
LIMIT = 65_800_000
```

```python
import functools

import jax
import jax.numpy as jnp
from jax import lax
from jax.experimental import pallas as pl
from jax.experimental.pallas import tpu as pltpu
from jax.sharding import PartitionSpec as P

MESH = pl.DeviceIdType.MESH
MEMBERS = 4
BLOCKS = [(0, 0), (0, 1), (1, 0), (3, 0), (2, 0), (2, 1), (1, 1), (3, 1)]
L, N1, O, N2 = range(4)
RING = 7
UNIT = 512
TILE = 512
F32 = jnp.float32
BF16 = jnp.bfloat16


def there(block):
    k, rel = BLOCKS[block]
    return BLOCKS.index(((MEMBERS - k) % MEMBERS, rel))


def dot(a, b):
    return jnp.dot(a, b, preferred_element_type=F32)


def kernel(slots, expert, slot, gate, x_hbm, wg, wu, wd, y_ref, zs, zr, h, orv, w1, w2,
           x_sem, w1_sem, w2_sem, zs_sem, zr_sem, os_sem, or_sem):
    tokens, d = y_ref.shape
    ff = h.shape[1]
    pair = 2 * slots
    units, tiles = ff // UNIT, d // TILE
    me, group = lax.axis_index("ep"), lax.axis_index("dp")
    core = lax.rem(group, 2)
    base = group - core
    cores = (core, 1 - core)

    def device(block):
        k, rel = BLOCKS[block]
        return {"ep": lax.rem(me + k, MEMBERS), "dp": base + cores[rel]}

    def first_code(block):
        k, rel = BLOCKS[block]
        return (2 * lax.rem(me + k, MEMBERS) + cores[rel]) * slots

    def rows(block):
        return pl.ds(block * slots, slots)

    def chunk(c):
        return slice(c * pair, (c + 1) * pair)

    def columns(t, width):
        return pl.ds(pl.multiple_of(t * width, width), width)

    def sent(c):
        return slice(c * pair - slots, (c + 1) * pair - slots)

    def hidden(c):
        return slice(0, pair) if c == L else slice(pair, 2 * pair)

    def x_copy(t):
        return pltpu.make_async_copy(x_hbm.at[:, columns(t, TILE)], y_ref.at[:, columns(t, TILE)], x_sem.at[t])

    def w1_start(unit, at):
        for i, w in enumerate((wg, wu)):
            pltpu.make_async_copy(w.at[core, :, columns(unit, UNIT)], w1.at[at, i], w1_sem.at[at, i]).start()

    def w1_wait(at):
        for i in range(2):
            pltpu.make_async_copy(w1.at[at, i], w1.at[at, i], w1_sem.at[at, i]).wait()

    def w2_copy(tile):
        return pltpu.make_async_copy(wd.at[core, :, columns(tile, TILE)], w2.at[tile], w2_sem.at[tile])

    def z_copy(block):
        return pltpu.make_async_remote_copy(
            src_ref=zs.at[rows(block - 1)],
            dst_ref=zr.at[rows(there(block))],
            send_sem=zs_sem.at[block],
            recv_sem=zr_sem.at[there(block)],
            device_id=device(block),
            device_id_type=MESH,
        )

    def o_copy(tile, block):
        return pltpu.make_async_remote_copy(
            src_ref=zs.at[rows(block - 1), columns(tile, TILE)],
            dst_ref=orv.at[tile, rows(there(block))],
            send_sem=os_sem.at[tile, block],
            recv_sem=or_sem.at[tile, there(block)],
            device_id=device(block),
            device_id_type=MESH,
        )

    def z_arrived(block):
        ref, sem = zr.at[rows(block)], zr_sem.at[block]
        pltpu.make_async_copy(ref, ref, sem).wait()

    def o_arrived(tile, block):
        ref, sem = orv.at[tile, rows(block)], or_sem.at[tile, block]
        pltpu.make_async_copy(ref, ref, sem).wait()

    for t in range(tiles):
        x_copy(t).start()
    barrier = pltpu.get_barrier_semaphore()
    for block in range(1, len(BLOCKS)):
        pl.semaphore_signal(barrier, inc=1, device_id=device(block), device_id_type=MESH)
    for p in range(RING):
        w1_start(p, p)

    code = jnp.where(slot[...] < slots, expert[...] * slots + slot[...], -1)

    def bases(index, c):
        return index + jnp.where(index < slots, first_code(2 * c), first_code(2 * c + 1) - slots)

    def dispatch(c):
        row = bases(lax.broadcasted_iota(jnp.int32, (pair, tokens), 0), c)
        pick = (code[0:1] == row) | (code[1:2] == row)
        pick = jnp.where(pick, 1.0, 0.0).astype(BF16)
        for t in range(tiles):
            if c == N1:
                x_copy(t).wait()
            at = slice(t * TILE, (t + 1) * TILE)
            z = dot(pick, y_ref[:, at]).astype(BF16)
            if c == L:
                zr[0:slots, at] = z[0:slots]
                zs[0:slots, at] = z[slots:pair]
            else:
                zs[sent(c), at] = z

    dispatch(N1)
    pl.semaphore_wait(barrier, len(BLOCKS) - 1)
    z_copy(2 * N1).start()
    z_copy(2 * N1 + 1).start()
    dispatch(L)
    dispatch(O)
    z_copy(2 * L + 1).start()
    z_copy(2 * O).start()
    z_copy(2 * O + 1).start()
    fresh = units - RING

    def project(at, unit, first, count, into):
        z = zr[first:first + count, :]
        a = dot(z, w1[at, 0])
        b = dot(z, w1[at, 1])
        h[into:into + count, columns(unit, UNIT)] = (a * jax.nn.sigmoid(a) * b).astype(BF16)

    def up_pass(turn, c):
        def place(p):
            return lax.rem(units * turn + p, RING)

        def unit_of(p):
            return lax.rem(p + fresh * turn, units)

        def step(i, _):
            for p in (2 * i, 2 * i + 1):
                pl.when(p >= RING)(functools.partial(w1_wait, place(p)))
            for p in (2 * i, 2 * i + 1):
                project(place(p), unit_of(p), c * pair, pair, pair)

            @pl.when(i < fresh // 2)
            def _():
                for p in (2 * i, 2 * i + 1):
                    w1_start(unit_of(p + RING), place(p))

            return 0

        lax.fori_loop(0, units // 2, step, 0)
        w1_wait(place(units - 1))
        project(place(units - 1), unit_of(units - 1), c * pair, pair, pair)

    def first_own(p, _):
        w1_wait(p)
        project(p, p, 0, pair, 0)
        return 0

    def first_near(i, _):
        for p in (2 * i, 2 * i + 1):
            project(p, p, pair, pair, pair)

        @pl.when(i < fresh // 2)
        def _():
            for p in (2 * i, 2 * i + 1):
                w1_start(p + RING, p)

        return 0

    def first_both(p, _):
        w1_wait(p)
        for c in (L, N1):
            project(p, p + RING, c * pair, pair, c * pair)

        @pl.when(p == SEND_N2)
        def _():
            z_copy(2 * N2).start()
            z_copy(2 * N2 + 1).start()

        return 0

    def down_pass(c, first=False):
        for block in (2 * c, 2 * c + 1):
            if block:
                z_copy(block).wait_send()

        for start in range(0, tiles, BATCH):
            batch = range(start, start + BATCH)
            for tile in batch:
                if first:
                    w2_copy(tile).wait()
            for tile in batch:
                out = dot(h[hidden(c), :], w2[tile]).astype(BF16)
                if c == L:
                    orv[tile, 0:slots, :] = out[0:slots]
                    zs[0:slots, columns(tile, TILE)] = out[slots:pair]
                else:
                    zs[sent(c), columns(tile, TILE)] = out
            for tile in batch:
                if c != L:
                    o_copy(tile, 2 * c).start()
                o_copy(tile, 2 * c + 1).start()

    def wait_z(c):
        z_arrived(2 * c)
        z_arrived(2 * c + 1)

    for tile in range(tiles):
        w2_copy(tile).start(priority=1)
    z_arrived(2 * L + 1)
    lax.fori_loop(0, RING, first_own, 0)
    dispatch(N2)

    wait_z(N1)
    lax.fori_loop(0, RING // 2, first_near, 0)
    project(RING - 1, RING - 1, pair, pair, pair)
    lax.fori_loop(0, fresh, first_both, 0)
    down_pass(N1, first=True)
    def weighs(c, part):
        half = tokens // 2
        at = (2 * c + part) * half * 2
        return slice(pair, pair + half), slice(at, at + pair)

    table = jnp.concatenate([code.astype(F32), gate[...], jnp.zeros((124, tokens), F32)], axis=0).T
    for c in range(4):
        column = bases(lax.broadcasted_iota(jnp.int32, (tokens, pair), 1), c).astype(F32)
        weight = jnp.where(table[:, 0:1] == column, table[:, 2:3], 0.0)
        weight = weight + jnp.where(table[:, 1:2] == column, table[:, 3:4], 0.0)
        weight = weight.astype(BF16)
        for part in range(2):
            zr[weighs(c, part)] = weight[part * (tokens // 2):(part + 1) * (tokens // 2)]

    wait_z(O)
    up_pass(1, O)
    down_pass(O)
    wait_z(N2)
    up_pass(2, N2)
    down_pass(N2)
    down_pass(L)

    for tile in range(tiles):
        for block in range(1, 2 * N2):
            o_arrived(tile, block)
        totals = []
        for part in range(2):
            total = dot(zr[weighs(0, part)], orv[tile, chunk(0), :])
            for c in range(1, N2):
                total = total + dot(zr[weighs(c, part)], orv[tile, chunk(c), :])
            totals.append(total)
        for block in (2 * N2, 2 * N2 + 1):
            o_arrived(tile, block)
        for part in range(2):
            total = totals[part] + dot(zr[weighs(N2, part)], orv[tile, chunk(N2), :])
            half = tokens // 2
            y_ref[part * half:(part + 1) * half, tile * TILE:(tile + 1) * TILE] = total.astype(BF16)

    for block in range(1, len(BLOCKS)):
        for tile in range(tiles):
            o_copy(tile, block).wait_send()


SEND_N2 = 1
BATCH = 1


def solution(mesh):
    def body(x, expert, slot, gate, w_gate, w_up, w_down):
        tokens, d = x.shape[2:]
        top = expert.shape[3]
        held, _, ff = w_gate.shape
        experts = held * mesh.shape["ep"]
        slots = 5 * tokens * top // (4 * experts)
        rows = experts * slots
        vmem = pl.BlockSpec(memory_space=pltpu.VMEM)
        hbm = pl.BlockSpec(memory_space=pltpu.HBM)
        tiles = d // TILE
        dma = pltpu.SemaphoreType.DMA
        y = pl.pallas_call(
            functools.partial(kernel, slots),
            name="moe",
            out_shape=OUT((tokens, d), BF16),
            in_specs=[vmem, vmem, vmem, hbm, hbm, hbm, hbm],
            out_specs=vmem,
            scratch_shapes=[
                pltpu.VMEM((rows - slots, d), BF16),
                pltpu.VMEM((rows, d), BF16),
                pltpu.VMEM((4 * slots, ff), BF16),
                pltpu.VMEM((tiles, rows, TILE), BF16),
                pltpu.VMEM((RING, 2, d, UNIT), BF16),
                pltpu.VMEM((tiles, ff, TILE), BF16),
                dma((tiles,)),
                dma((RING, 2)),
                dma((tiles,)),
                dma((8,)),
                dma((8,)),
                dma((tiles, 8)),
                dma((tiles, 8)),
            ],
            compiler_params=pltpu.CompilerParams(
                collective_id=0, has_side_effects=True, vmem_limit_bytes=LIMIT
            ),
        )(expert[0, 0].T, slot[0, 0].T, gate[0, 0].T, x[0, 0], w_gate, w_up, w_down)
        return y[None, None]

    part = P("dp", "ep")
    weights = P("ep")
    return jax.shard_map(
        body, mesh=mesh, in_specs=(part, part, part, part, weights, weights, weights), out_specs=part, check_vma=False
    )


OUT = pltpu.VMEM
LIMIT = 65_800_000
```
